32 devices in a mesh: gx: 4 (over x, core), gy: 2 (over y), gz: 4 (over z).
Axes of the slice: x: 2, y: 2, z: 4, core: 2. Of those that a mesh axis runs over, the one named last changes fastest.
Arguments:
- displace: float32 [3, 8, 16, 512], P(None, 'gx', 'gy', 'gz'), may hold values from -0.15 to 0.15
- occupied: int32 [8, 16, 512], P('gx', 'gy', 'gz'), may hold values from 0 to 1, as said below
- strength: float32 [8, 16, 512], P('gx', 'gy', 'gz'), may hold values from 0.5 to 2
Outputs:
- force: float32 [3, 8, 16, 512], P(None, 'gx', 'gy', 'gz')
- energy: float32 [8, 16, 512], P('gx', 'gy', 'gz')
The draws below stay inside these ranges and needn't reach their ends.
Inputs may be any that keep to these rules, and one draw needn't show every extreme that they name: `occupied`: 0 for a vacancy, 1 for an atom; the share of vacancies differs from domain to domain.
All inputs are finite; a program needn't handle non-finite values.
Results may differ from the reference program's by a relative error of at most 0.00017.
Values sent between devices are 32-bit elements; how exact they have to be, the bound alone decides.
A program may use at most 64 MiB of HBM per device.

```python
import math
import jax
import jax.numpy as jnp
from jax import lax

CX = 2
CY = 8
CZ = 128
ITERS = 3
NX = 8
NY = 16
NZ = 512


def draw_occupied(key, part):
    rate_key, site_key = jax.random.split(jax.random.fold_in(key, 17))
    domains = jax.random.randint(rate_key, (NX // CX, NY // CY, NZ // CZ), 50, 96)
    domain_rate = jnp.repeat(jnp.repeat(jnp.repeat(domains, CX, axis=0), CY, axis=1), CZ, axis=2)
    dice_rolls = jax.random.randint(site_key, (NX, NY, NZ), 0, 100)
    return (dice_rolls < domain_rate).astype(jnp.int32)


def shard_levels(stream_key, extent, cuts, low, high):
    def one(axis_at, blocks):
        heights = jax.random.uniform(jax.random.fold_in(jax.random.fold_in(stream_key, 6), axis_at), (blocks,), jnp.float32, low / len(cuts), high / len(cuts))
        return jnp.repeat(jnp.exp(heights), extent[axis_at] // blocks).reshape((-1,) + (1,) * (len(extent) - axis_at - 1))

    factor_of = one(*cuts[0])
    for cut in cuts[1:]:
        factor_of = factor_of * one(*cut)
    return factor_of


def noise(own_key, shape, width, most, cuts=(), kind=jnp.bfloat16):
    values = jax.random.normal(own_key, shape, jnp.float32) * width
    if len(cuts) > 0:
        values = shard_levels(own_key, shape, cuts, -0.22, 0.18) * values
    return jnp.clip(values, min=-most, max=most).astype(kind)


def setup_inputs(seed: int = 0) -> dict:
    seeds = jax.random.split(jax.random.key(seed), 4)
    displace = noise(seeds[0], (3, NX, NY, NZ), 0.05, 0.15, ((1, 4), (2, 2), (3, 4)), jnp.float32)
    occupied = draw_occupied(jax.random.fold_in(seeds[3], 71), 0)
    strength = jnp.clip(jnp.exp(math.log(2.0) - 1.3862944 * jax.random.uniform(seeds[2], (NX, NY, NZ), jnp.float32) ** shard_levels(seeds[2], (NX, NY, NZ), ((0, 4), (1, 2), (2, 4)), -0.2, 0.2)), 0.5, 2.0)
    return dict(displace=displace, occupied=occupied, strength=strength)


RADIUS_SQ = 4.84
STEP = 0.02

def cutoff(distance):
    inside = 1.0 - distance * distance / RADIUS_SQ
    return inside * inside

def cutoff_slope(distance):
    inside = 1.0 - distance * distance / RADIUS_SQ
    return -4.0 * inside * distance / RADIUS_SQ

def density(distance):
    return jnp.exp(-2.0 * (distance - 1.0)) * cutoff(distance)

def density_slope(distance):
    growth = jnp.exp(-2.0 * (distance - 1.0))
    return growth * (cutoff_slope(distance) - 2.0 * cutoff(distance))

def repulse(distance):
    return 0.5 * jnp.exp(-4.0 * (distance - 1.0)) * cutoff(distance)

def repulse_slope(distance):
    growth = 0.5 * jnp.exp(-4.0 * (distance - 1.0))
    return growth * (cutoff_slope(distance) - 4.0 * cutoff(distance))
FULL_OFFSETS = [(first, second, third) for first in (-1, 0, 1) for second in (-1, 0, 1) for third in (-1, 0, 1) if (first, second, third) != (0, 0, 0)]

def neighbour(padded, offset):
    return padded[..., 1 + offset[0]:1 + offset[0] + NX, 1 + offset[1]:1 + offset[1] + NY, 1 + offset[2]:1 + offset[2] + NZ]

def evaluate(displace, occupancy, weight):
    pad_disp = jnp.pad(displace, ((0, 0), (1, 1), (1, 1), (1, 1)))
    pad_weight = jnp.pad(weight, 1)

    def geometry(offset):
        lattice = jnp.array(offset, jnp.float32).reshape(3, 1, 1, 1)
        separation = lattice + neighbour(pad_disp, offset) - displace
        distance = jnp.sqrt(lax.optimization_barrier(jnp.sum(separation * separation, axis=0)))
        return (separation, distance)
    density_sum = jnp.zeros(weight.shape, jnp.float32)
    for offset in FULL_OFFSETS:
        separation, distance = geometry(offset)
        density_sum = density_sum + neighbour(pad_weight, offset) * density(distance)
    slope = occupancy * -0.5 / jnp.sqrt(1.0 + density_sum)
    pad_slope = jnp.pad(slope, 1)
    force = jnp.zeros(displace.shape, jnp.float32)
    pair_sum = jnp.zeros(weight.shape, jnp.float32)
    for offset in FULL_OFFSETS:
        separation, distance = geometry(offset)
        near_weight = neighbour(pad_weight, offset)
        near_slope = neighbour(pad_slope, offset)
        coupling = (slope * near_weight + near_slope * weight) * density_slope(distance) + weight * near_weight * repulse_slope(distance)
        force = force + coupling / distance * separation
        pair_sum = pair_sum + near_weight * repulse(distance)
    energy = occupancy * -jnp.sqrt(1.0 + density_sum) + 0.5 * weight * pair_sum
    return (force, energy)

def reference(displace, occupied, strength):
    occupancy = occupied.astype(jnp.float32)
    weight = occupancy * strength
    current = displace
    force, energy = evaluate(current, occupancy, weight)
    for step in range(ITERS - 1):
        current = current + STEP * force
        force, energy = evaluate(current, occupancy, weight)
    return (force, energy)
```

```python
import functools

import jax
import jax.numpy as jnp
from jax import lax
from jax.experimental import pallas as pl
from jax.experimental.pallas import tpu as pltpu
from jax.sharding import PartitionSpec as P

ITERS = 3
RADIUS_SQ = 4.84
STEP = 0.02
AXES = ("gx", "gy", "gz")
MESH = pl.DeviceIdType.MESH
LANES = 128
PLANE = [(dx, dy) for dx in (-1, 0, 1) for dy in (-1, 0, 1)]
NEAR = sorted(
    ((dx, dy, dz) for dx, dy in PLANE for dz in (-1, 0, 1) if (dx, dy, dz) != (0, 0, 0)),
    key=lambda o: (-sum(abs(a) for a in o), o),
)
SLOT = {o: i for i, o in enumerate(NEAR)}


def minus(o):
    return tuple(-a for a in o)


def up(rows):
    return -(-rows // 8) * 8


def kernel(sizes, counts, disp_ref, occ_ref, str_ref, force_ref, energy_ref,
           xs, ys, zs, xl, yl, zl, stage, near, cols, slopes, send_sem, recv_sem):
    cx, cy, cz = sizes
    pitch = cy + 4
    group = LANES // 4
    xu, yu = 3 * cx * cy, 3 * cx * 2
    xpanel, ypanel = xu, yu
    xw, yw = up(xu + 2), up(yu + 2)
    x_rows = (xs.shape[1], xw)
    y_rows = (ys.shape[2], yw)

    me = [lax.axis_index(axis) for axis in AXES]
    there = [[None if s == 0 else (m + s >= 0) & (m + s < n) for s in (-1, 0, 1)]
             for m, n in zip(me, counts)]

    def exists(o):
        tests = [there[a][o[a] + 1] for a in range(3) if o[a] != 0]
        return functools.reduce(lambda p, q: p & q, tests)

    def target(o):
        return {AXES[a]: me[a] + o[a] for a in range(3)}

    barrier = pltpu.get_barrier_semaphore()
    for o in NEAR:
        @pl.when(exists(o))
        def _(o=o):
            pl.semaphore_signal(barrier, inc=1, device_id=target(o), device_id_type=MESH)
    spans = [1 + (m > 0).astype(jnp.int32) + (m < n - 1).astype(jnp.int32)
             for m, n in zip(me, counts)]

    def ends(t, o):
        back = minus(o)
        if o[2] != 0:
            side = 0 if o[2] == 1 else 1
            src = zs.at[t, side]
            dst = zl.at[t, PLANE.index(back[:2]), side]
        elif o[1] != 0:
            rows = y_rows[0] if t == 0 else y_rows[1]
            side = 0 if o[1] == 1 else 1
            src = ys.at[t, side, pl.ds(0, rows)]
            dst = yl.at[t, back[0] + 1, side, pl.ds(0, rows)]
        else:
            rows = x_rows[0] if t == 0 else x_rows[1]
            src = xs.at[t, pl.ds(0, rows)]
            dst = xl.at[t, 0 if o[0] == 1 else 1, pl.ds(0, rows)]
        return pltpu.make_async_remote_copy(
            src_ref=src, dst_ref=dst, send_sem=send_sem.at[t, SLOT[o]],
            recv_sem=recv_sem.at[t, SLOT[back]], device_id=target(o), device_id_type=MESH)

    for o in NEAR:
        @pl.when(jnp.logical_not(exists(o)))
        def _(o=o):
            if o[2] != 0:
                spot = zl.at[:, PLANE.index(o[:2]), 0 if o[2] == -1 else 1]
            elif o[1] != 0:
                spot = yl.at[:, o[0] + 1, 0 if o[1] == -1 else 1]
            else:
                spot = xl.at[:, 0 if o[0] == -1 else 1]
            spot[...] = jnp.zeros(spot.shape, jnp.float32)

    stage[...] = jnp.zeros(stage.shape, jnp.float32)
    near[...] = jnp.zeros(near.shape, jnp.float32)
    cols[...] = jnp.zeros(cols.shape, jnp.float32)

    mine = [[disp_ref[q, x] for x in range(cx)] for q in range(3)]
    mine.append([occ_ref[x].astype(jnp.float32) * str_ref[x] for x in range(cx)])

    lane = lax.broadcasted_iota(jnp.int32, (8, LANES), 1)
    sub = lax.broadcasted_iota(jnp.int32, (8, LANES), 0)
    in_group = lax.rem(lax.rem(lane, group), pitch)
    depth = (lax.rem(sub, 4) - 1).astype(jnp.float32)
    middle = lax.rem(sub, 4) == 1
    hollow = lax.rem(sub, 4) == 3

    def moved(value, amount, axis=1):
        amount %= value.shape[axis]
        return value if amount == 0 else pltpu.roll(value, amount, axis)

    for t in range(ITERS):
        last = t == ITERS - 1
        for q in range(4):
            for x in range(cx):
                if q < 3 or t == 0:
                    stage[q * group + x * pitch + 2:q * group + x * pitch + 2 + cy] = mine[q][x]
        flipped = jnp.transpose(stage[...])
        head, tail = flipped[0:2], flipped[cz - 2:cz]
        first, final = flipped[0:1], flipped[cz - 1:cz]
        zs[t, 0] = tail
        zs[t, 1] = head
        for side in range(2):
            for q in range(4):
                if q == 3 and t > 0:
                    continue
                for x in range(cx):
                    base = (q * cx + x) * 2 if q < 3 else yw + x * 2
                    piece = mine[q][x]
                    ys[t, side, base:base + 2] = piece[cy - 2:cy] if side == 0 else piece[0:2]
            ys[t, side, ypanel:ypanel + 1] = first
            ys[t, side, ypanel + 1:ypanel + 2] = final
        for q in range(4):
            if q == 3 and t > 0:
                continue
            for x in range(cx):
                base = (q * cx + x) * cy if q < 3 else xw + x * cy
                xs[t, base:base + cy] = mine[q][x]
        xs[t, xpanel:xpanel + 1] = first
        xs[t, xpanel + 1:xpanel + 2] = final

        if t == 0:
            pl.semaphore_wait(barrier, spans[0] * spans[1] * spans[2] - 1)
        for o in NEAR:
            @pl.when(exists(o))
            def _(o=o):
                ends(t, o).start()
        for o in reversed(NEAR):
            @pl.when(exists(o))
            def _(o=o):
                ends(t, minus(o)).wait_recv()

        quantities = range(4) if t == 0 else range(3)
        for q in quantities:
            for dx in (-1, 0, 1):
                for x in range(cx):
                    row = (cx * (dx + 1) + x) * pitch
                    if dx == 0:
                        piece = mine[q][x]
                    else:
                        base = (q * cx + x) * cy if q < 3 else xw + x * cy
                        piece = xl[t, 0 if dx == -1 else 1, base:base + cy]
                    near[1, q, row + 2:row + 2 + cy] = piece
                    base = (q * cx + x) * 2 if q < 3 else yw + x * 2
                    near[1, q, row:row + 2] = yl[t, dx + 1, 0, base:base + 2]
                    near[1, q, row + 2 + cy:row + 4 + cy] = yl[t, dx + 1, 1, base:base + 2]
        for j, (dx, dy) in enumerate(PLANE):
            cols[j, 0:2] = zl[t, j, 0]
            cols[j, 5:7] = zl[t, j, 1]
            if dy != 0:
                a = yl[t, dx + 1, 0 if dy == -1 else 1, ypanel:ypanel + 1]
                b = yl[t, dx + 1, 0 if dy == -1 else 1, ypanel + 1:ypanel + 2]
            elif dx != 0:
                a = xl[t, 0 if dx == -1 else 1, xpanel:xpanel + 1]
                b = xl[t, 0 if dx == -1 else 1, xpanel + 1:xpanel + 2]
            else:
                a, b = first, final
            cols[j, 2:3] = a
            cols[j, 4:5] = b
        joined = []
        for dx in (-1, 0, 1):
            low, mid, high = (cols[PLANE.index((dx, dy))] for dy in (-1, 0, 1))
            joined.append(jnp.where(in_group < 2, moved(low, -cy),
                                    jnp.where(in_group < 2 + cy, mid, moved(high, cy))))
        wide = cx * pitch
        edge = []
        for q in range(4):
            value = jnp.zeros((8, LANES), jnp.float32)
            for i in (2, 1, 0):
                value = jnp.where(lane < wide * (i + 1),
                                  moved(joined[i], wide * i - group * q),
                                  value if i < 2 else 0.0)
            edge.append(value)

        turned = jnp.transpose(jnp.concatenate(edge, axis=0))
        rows = near.shape[2]
        wide_lane = lax.broadcasted_iota(jnp.int32, (rows, LANES), 1)
        for q in quantities:
            here = near[1, q]
            before = turned[0:rows, 8 * q + 1:8 * q + 2]
            after = turned[0:rows, 8 * q + 5:8 * q + 6]
            near[0, q] = jnp.where(wide_lane == 0, before, moved(here, 1))
            near[2, q] = jnp.where(wide_lane == cz - 1, after, moved(here, -1))

        center = [jnp.where(sub < 4, e[1:2], e[5:6]) for e in edge[:3]]
        total = jnp.zeros((8, LANES), jnp.float32)
        for dx, dy in PLANE:
            shift = -(dx * pitch + dy)
            far = [moved(e, shift) for e in edge]
            sx = far[0] - (center[0] - dx)
            sy = far[1] - (center[1] - dy)
            sz = far[2] - (center[2] - depth)
            square = sx * sx + sy * sy + sz * sz
            far_weight = far[3]
            if (dx, dy) == (0, 0):
                square = jnp.where(middle | hollow, 1.0, square)
                far_weight = jnp.where(middle | hollow, 0.0, far_weight)
            distance = square * lax.rsqrt(square)
            inside = 1.0 - square * (1.0 / RADIUS_SQ)
            total = total + far_weight * (jnp.exp(2.0 - 2.0 * distance) * (inside * inside))
        total = total + moved(total, 1, 0) + moved(total, -1, 0)
        edge_slope = jnp.where((edge[3] > 0.0) & middle, -0.5 * lax.rsqrt(1.0 + total), 0.0)
        turned_slope = jnp.transpose(edge_slope)

        begin = pitch + 1
        chunk = 16
        extent = up((cx + 2) * pitch + cy + 3 - begin)
        for start in range(begin, begin + extent, chunk):
            size = min(chunk, begin + extent - start)
            base = [[near[1, q, start:start + size] - s for s in (-1.0, 0.0, 1.0)] for q in range(3)]
            total = jnp.zeros((size, LANES), jnp.float32)
            for dx, dy in PLANE:
                row = start + dx * pitch + dy
                for dz in (-1, 0, 1):
                    if (dx, dy, dz) == (0, 0, 0):
                        continue
                    sx = near[dz + 1, 0, row:row + size] - base[0][dx + 1]
                    sy = near[dz + 1, 1, row:row + size] - base[1][dy + 1]
                    sz = near[dz + 1, 2, row:row + size] - base[2][dz + 1]
                    square = sx * sx + sy * sy + sz * sz
                    distance = square * lax.rsqrt(square)
                    inside = 1.0 - square * (1.0 / RADIUS_SQ)
                    total = total + near[dz + 1, 3, row:row + size] * (
                        jnp.exp(2.0 - 2.0 * distance) * (inside * inside))
            root = lax.rsqrt(1.0 + total)
            slope = jnp.where(near[1, 3, start:start + size] > 0.0, -0.5 * root, 0.0)
            slopes[1, start:start + size] = slope
            tall = lax.broadcasted_iota(jnp.int32, (size, LANES), 1)
            slopes[0, start:start + size] = jnp.where(
                tall == 0, turned_slope[start:start + size, 1:2], moved(slope, 1))
            slopes[2, start:start + size] = jnp.where(
                tall == cz - 1, turned_slope[start:start + size, 5:6], moved(slope, -1))
            if last:
                slopes[3, start:start + size] = (1.0 + total) * root

        for x in range(cx):
            start = (cx + x) * pitch + 2
            here = [mine[q][x] for q in range(3)]
            base = [[h - s for s in (-1.0, 0.0, 1.0)] for h in here]
            weight = mine[3][x]
            slope = slopes[1, start:start + cy]
            force = [jnp.zeros((cy, LANES), jnp.float32) for _ in range(3)]
            pair = jnp.zeros((cy, LANES), jnp.float32)
            for dx, dy in PLANE:
                row = start + dx * pitch + dy
                for dz in (-1, 0, 1):
                    if (dx, dy, dz) == (0, 0, 0):
                        continue
                    sx = near[dz + 1, 0, row:row + cy] - base[0][dx + 1]
                    sy = near[dz + 1, 1, row:row + cy] - base[1][dy + 1]
                    sz = near[dz + 1, 2, row:row + cy] - base[2][dz + 1]
                    far_weight = near[dz + 1, 3, row:row + cy]
                    far_slope = slopes[dz + 1, row:row + cy]
                    square = sx * sx + sy * sy + sz * sz
                    inverse = lax.rsqrt(square)
                    distance = square * inverse
                    inside = 1.0 - square * (1.0 / RADIUS_SQ)
                    cut = inside * inside
                    cut_slope = inside * distance * (-4.0 / RADIUS_SQ)
                    growth = jnp.exp(2.0 - 2.0 * distance)
                    steep = 0.5 * growth * growth
                    coupling = (slope * far_weight + far_slope * weight) * (
                        growth * (cut_slope - 2.0 * cut)) + weight * far_weight * (
                        steep * (cut_slope - 4.0 * cut))
                    scale = coupling * inverse
                    force = [force[0] + scale * sx, force[1] + scale * sy, force[2] + scale * sz]
                    if last:
                        pair = pair + far_weight * (steep * cut)
            if last:
                for q in range(3):
                    force_ref[q, x] = force[q]
                energy_ref[x] = 0.5 * weight * pair - jnp.where(
                    weight > 0.0, slopes[3, start:start + cy], 0.0)
            else:
                for q in range(3):
                    mine[q][x] = here[q] + STEP * force[q]

    for t in range(ITERS):
        for o in NEAR:
            @pl.when(exists(o))
            def _(o=o, t=t):
                ends(t, o).wait_send()


def solution(mesh):
    counts = tuple(mesh.shape[axis] for axis in AXES)

    def body(displace, occupied, strength):
        sizes = occupied.shape
        cx, cy, cz = sizes
        pitch = cy + 4
        x_rows = up(3 * cx * cy + 2) + up(cx * cy)
        y_rows = up(6 * cx + 2) + up(2 * cx)
        rows = up(2 * (pitch + 1) + up((cx + 2) * pitch + cy + 3 - (pitch + 1)))
        f32 = jnp.float32
        vmem = pl.BlockSpec(memory_space=pltpu.VMEM)
        return pl.pallas_call(
            functools.partial(kernel, sizes, counts),
            out_shape=(jax.ShapeDtypeStruct((3,) + sizes, f32), jax.ShapeDtypeStruct(sizes, f32)),
            in_specs=[vmem] * 3,
            out_specs=(vmem, vmem),
            scratch_shapes=[
                pltpu.VMEM((ITERS, x_rows, LANES), f32),
                pltpu.VMEM((ITERS, 2, y_rows, LANES), f32),
                pltpu.VMEM((ITERS, 2, 2, LANES), f32),
                pltpu.VMEM((ITERS, 2, x_rows, LANES), f32),
                pltpu.VMEM((ITERS, 3, 2, y_rows, LANES), f32),
                pltpu.VMEM((ITERS, 9, 2, 2, LANES), f32),
                pltpu.VMEM((LANES, LANES), f32),
                pltpu.VMEM((3, 4, rows, LANES), f32),
                pltpu.VMEM((9, 8, LANES), f32),
                pltpu.VMEM((4, rows, LANES), f32),
                pltpu.SemaphoreType.DMA((ITERS, len(NEAR))),
                pltpu.SemaphoreType.DMA((ITERS, len(NEAR))),
            ],
            compiler_params=pltpu.CompilerParams(collective_id=0, has_side_effects=True),
        )(displace, occupied, strength)

    in_specs = (P(None, "gx", "gy", "gz"), P("gx", "gy", "gz"), P("gx", "gy", "gz"))
    out_specs = (P(None, "gx", "gy", "gz"), P("gx", "gy", "gz"))
    return jax.shard_map(body, mesh=mesh, in_specs=in_specs, out_specs=out_specs, check_vma=False)
```

```python
import functools

import jax
import jax.numpy as jnp
from jax import lax
from jax.experimental import pallas as pl
from jax.experimental.pallas import tpu as pltpu
from jax.sharding import PartitionSpec as P

ITERS = 3
RADIUS_SQ = 4.84
STEP = 0.02
AXES = ("gx", "gy", "gz")
MESH = pl.DeviceIdType.MESH
LANES = 128
PLANE = [(dx, dy) for dx in (-1, 0, 1) for dy in (-1, 0, 1)]
NEAR = sorted(
    ((dx, dy, dz) for dx, dy in PLANE for dz in (-1, 0, 1) if (dx, dy, dz) != (0, 0, 0)),
    key=lambda o: (-sum(abs(a) for a in o), o),
)
SLOT = {o: i for i, o in enumerate(NEAR)}


def minus(o):
    return tuple(-a for a in o)


def up(rows):
    return -(-rows // 8) * 8


def kernel(sizes, counts, disp_hbm, occ_hbm, str_hbm, force_ref, energy_ref,
           xs, ys, zs, xl, yl, zl, stage, near, cols, slopes, disp_ref, occ_ref, str_ref,
           send_sem, recv_sem, load_sem):
    cx, cy, cz = sizes
    pitch = cy + 4
    group = LANES // 4
    xu, yu = 3 * cx * cy, 3 * cx * 2
    xpanel, ypanel = xu, yu
    xw, yw = up(xu + 2), up(yu + 2)
    x_rows = (xs.shape[1], xw)
    y_rows = (ys.shape[2], yw)

    loads = [pltpu.make_async_copy(disp_hbm, disp_ref, load_sem.at[0]),
             pltpu.make_async_copy(occ_hbm, occ_ref, load_sem.at[1]),
             pltpu.make_async_copy(str_hbm, str_ref, load_sem.at[2])]
    for load in loads:
        load.start()

    me = [lax.axis_index(axis) for axis in AXES]
    there = [[None if s == 0 else (m + s >= 0) & (m + s < n) for s in (-1, 0, 1)]
             for m, n in zip(me, counts)]

    def exists(o):
        tests = [there[a][o[a] + 1] for a in range(3) if o[a] != 0]
        return functools.reduce(lambda p, q: p & q, tests)

    def target(o):
        return {AXES[a]: me[a] + o[a] for a in range(3)}

    barrier = pltpu.get_barrier_semaphore()
    for o in NEAR:
        @pl.when(exists(o))
        def _(o=o):
            pl.semaphore_signal(barrier, inc=1, device_id=target(o), device_id_type=MESH)
    spans = [1 + (m > 0).astype(jnp.int32) + (m < n - 1).astype(jnp.int32)
             for m, n in zip(me, counts)]

    def ends(t, o):
        back = minus(o)
        if o[2] != 0:
            side = 0 if o[2] == 1 else 1
            src = zs.at[t, side]
            dst = zl.at[t, PLANE.index(back[:2]), side]
        elif o[1] != 0:
            rows = y_rows[0] if t == 0 else y_rows[1]
            side = 0 if o[1] == 1 else 1
            src = ys.at[t, side, pl.ds(0, rows)]
            dst = yl.at[t, back[0] + 1, side, pl.ds(0, rows)]
        else:
            rows = x_rows[0] if t == 0 else x_rows[1]
            src = xs.at[t, pl.ds(0, rows)]
            dst = xl.at[t, 0 if o[0] == 1 else 1, pl.ds(0, rows)]
        return pltpu.make_async_remote_copy(
            src_ref=src, dst_ref=dst, send_sem=send_sem.at[SLOT[o]],
            recv_sem=recv_sem.at[t % 2, SLOT[back]], device_id=target(o), device_id_type=MESH)

    for o in NEAR:
        @pl.when(jnp.logical_not(exists(o)))
        def _(o=o):
            if o[2] != 0:
                spot = zl.at[:, PLANE.index(o[:2]), 0 if o[2] == -1 else 1]
            elif o[1] != 0:
                spot = yl.at[:, o[0] + 1, 0 if o[1] == -1 else 1]
            else:
                spot = xl.at[:, 0 if o[0] == -1 else 1]
            spot[...] = jnp.zeros(spot.shape, jnp.float32)

    stage[...] = jnp.zeros(stage.shape, jnp.float32)
    near[...] = jnp.zeros(near.shape, jnp.float32)
    cols[...] = jnp.zeros(cols.shape, jnp.float32)

    for load in loads:
        load.wait()
    mine = [[disp_ref[q, x] for x in range(cx)] for q in range(3)]
    mine.append([occ_ref[x].astype(jnp.float32) * str_ref[x] for x in range(cx)])

    lane = lax.broadcasted_iota(jnp.int32, (8, LANES), 1)
    sub = lax.broadcasted_iota(jnp.int32, (8, LANES), 0)
    in_group = lax.rem(lax.rem(lane, group), pitch)
    depth = (lax.rem(sub, 4) - 1).astype(jnp.float32)
    middle = lax.rem(sub, 4) == 1
    hollow = lax.rem(sub, 4) == 3

    def moved(value, amount, axis=1):
        amount %= value.shape[axis]
        return value if amount == 0 else pltpu.roll(value, amount, axis)

    for t in range(ITERS):
        last = t == ITERS - 1
        for q in range(4):
            for x in range(cx):
                if q < 3 or t == 0:
                    stage[q * group + x * pitch + 2:q * group + x * pitch + 2 + cy] = mine[q][x]
        flipped = jnp.transpose(stage[...])
        head, tail = flipped[0:2], flipped[cz - 2:cz]
        first, final = flipped[0:1], flipped[cz - 1:cz]
        zs[t, 0] = tail
        zs[t, 1] = head
        for side in range(2):
            for q in range(4):
                if q == 3 and t > 0:
                    continue
                for x in range(cx):
                    base = (q * cx + x) * 2 if q < 3 else yw + x * 2
                    piece = mine[q][x]
                    ys[t, side, base:base + 2] = piece[cy - 2:cy] if side == 0 else piece[0:2]
            ys[t, side, ypanel:ypanel + 1] = first
            ys[t, side, ypanel + 1:ypanel + 2] = final
        for q in range(4):
            if q == 3 and t > 0:
                continue
            for x in range(cx):
                base = (q * cx + x) * cy if q < 3 else xw + x * cy
                xs[t, base:base + cy] = mine[q][x]
        xs[t, xpanel:xpanel + 1] = first
        xs[t, xpanel + 1:xpanel + 2] = final

        if t == 0:
            pl.semaphore_wait(barrier, spans[0] * spans[1] * spans[2] - 1)
        for o in NEAR:
            @pl.when(exists(o))
            def _(o=o):
                ends(t, o).start()
        for o in reversed(NEAR):
            @pl.when(exists(o))
            def _(o=o):
                ends(t, minus(o)).wait_recv()
                ends(t, o).wait_send()

        quantities = range(4) if t == 0 else range(3)
        for q in quantities:
            for dx in (-1, 0, 1):
                for x in range(cx):
                    row = (cx * (dx + 1) + x) * pitch
                    if dx == 0:
                        piece = mine[q][x]
                    else:
                        base = (q * cx + x) * cy if q < 3 else xw + x * cy
                        piece = xl[t, 0 if dx == -1 else 1, base:base + cy]
                    near[1, q, row + 2:row + 2 + cy] = piece
                    base = (q * cx + x) * 2 if q < 3 else yw + x * 2
                    near[1, q, row:row + 2] = yl[t, dx + 1, 0, base:base + 2]
                    near[1, q, row + 2 + cy:row + 4 + cy] = yl[t, dx + 1, 1, base:base + 2]
        for j, (dx, dy) in enumerate(PLANE):
            cols[j, 0:2] = zl[t, j, 0]
            cols[j, 5:7] = zl[t, j, 1]
            if dy != 0:
                a = yl[t, dx + 1, 0 if dy == -1 else 1, ypanel:ypanel + 1]
                b = yl[t, dx + 1, 0 if dy == -1 else 1, ypanel + 1:ypanel + 2]
            elif dx != 0:
                a = xl[t, 0 if dx == -1 else 1, xpanel:xpanel + 1]
                b = xl[t, 0 if dx == -1 else 1, xpanel + 1:xpanel + 2]
            else:
                a, b = first, final
            cols[j, 2:3] = a
            cols[j, 4:5] = b
        joined = []
        for dx in (-1, 0, 1):
            low, mid, high = (cols[PLANE.index((dx, dy))] for dy in (-1, 0, 1))
            joined.append(jnp.where(in_group < 2, moved(low, -cy),
                                    jnp.where(in_group < 2 + cy, mid, moved(high, cy))))
        wide = cx * pitch
        edge = []
        for q in range(4):
            value = jnp.zeros((8, LANES), jnp.float32)
            for i in (2, 1, 0):
                value = jnp.where(lane < wide * (i + 1),
                                  moved(joined[i], wide * i - group * q),
                                  value if i < 2 else 0.0)
            edge.append(value)

        turned = jnp.transpose(jnp.concatenate(edge, axis=0))
        rows = near.shape[2]
        wide_lane = lax.broadcasted_iota(jnp.int32, (rows, LANES), 1)
        for q in quantities:
            here = near[1, q]
            before = turned[0:rows, 8 * q + 1:8 * q + 2]
            after = turned[0:rows, 8 * q + 5:8 * q + 6]
            near[0, q] = jnp.where(wide_lane == 0, before, moved(here, 1))
            near[2, q] = jnp.where(wide_lane == cz - 1, after, moved(here, -1))

        center = [jnp.where(sub < 4, e[1:2], e[5:6]) for e in edge[:3]]
        total = jnp.zeros((8, LANES), jnp.float32)
        for dx, dy in PLANE:
            shift = -(dx * pitch + dy)
            far = [moved(e, shift) for e in edge]
            sx = far[0] - (center[0] - dx)
            sy = far[1] - (center[1] - dy)
            sz = far[2] - (center[2] - depth)
            square = sx * sx + sy * sy + sz * sz
            far_weight = far[3]
            if (dx, dy) == (0, 0):
                square = jnp.where(middle | hollow, 1.0, square)
                far_weight = jnp.where(middle | hollow, 0.0, far_weight)
            distance = square * lax.rsqrt(square)
            inside = 1.0 - square * (1.0 / RADIUS_SQ)
            total = total + far_weight * (jnp.exp(2.0 - 2.0 * distance) * (inside * inside))
        total = total + moved(total, 1, 0) + moved(total, -1, 0)
        edge_slope = jnp.where((edge[3] > 0.0) & middle, -0.5 * lax.rsqrt(1.0 + total), 0.0)
        turned_slope = jnp.transpose(edge_slope)

        begin = pitch + 1
        chunk = 16
        extent = up((cx + 2) * pitch + cy + 3 - begin)
        for start in range(begin, begin + extent, chunk):
            size = min(chunk, begin + extent - start)
            base = [[near[1, q, start:start + size] - s for s in (-1.0, 0.0, 1.0)] for q in range(3)]
            total = jnp.zeros((size, LANES), jnp.float32)
            for dx, dy in PLANE:
                row = start + dx * pitch + dy
                for dz in (-1, 0, 1):
                    if (dx, dy, dz) == (0, 0, 0):
                        continue
                    sx = near[dz + 1, 0, row:row + size] - base[0][dx + 1]
                    sy = near[dz + 1, 1, row:row + size] - base[1][dy + 1]
                    sz = near[dz + 1, 2, row:row + size] - base[2][dz + 1]
                    square = sx * sx + sy * sy + sz * sz
                    distance = square * lax.rsqrt(square)
                    inside = 1.0 - square * (1.0 / RADIUS_SQ)
                    total = total + near[dz + 1, 3, row:row + size] * (
                        jnp.exp(2.0 - 2.0 * distance) * (inside * inside))
            root = lax.rsqrt(1.0 + total)
            slope = jnp.where(near[1, 3, start:start + size] > 0.0, -0.5 * root, 0.0)
            slopes[1, start:start + size] = slope
            tall = lax.broadcasted_iota(jnp.int32, (size, LANES), 1)
            slopes[0, start:start + size] = jnp.where(
                tall == 0, turned_slope[start:start + size, 1:2], moved(slope, 1))
            slopes[2, start:start + size] = jnp.where(
                tall == cz - 1, turned_slope[start:start + size, 5:6], moved(slope, -1))
            if last:
                slopes[3, start:start + size] = (1.0 + total) * root

        for x in range(cx):
            start = (cx + x) * pitch + 2
            here = [mine[q][x] for q in range(3)]
            base = [[h - s for s in (-1.0, 0.0, 1.0)] for h in here]
            weight = mine[3][x]
            slope = slopes[1, start:start + cy]
            force = [jnp.zeros((cy, LANES), jnp.float32) for _ in range(3)]
            pair = jnp.zeros((cy, LANES), jnp.float32)
            for dx, dy in PLANE:
                row = start + dx * pitch + dy
                for dz in (-1, 0, 1):
                    if (dx, dy, dz) == (0, 0, 0):
                        continue
                    sx = near[dz + 1, 0, row:row + cy] - base[0][dx + 1]
                    sy = near[dz + 1, 1, row:row + cy] - base[1][dy + 1]
                    sz = near[dz + 1, 2, row:row + cy] - base[2][dz + 1]
                    far_weight = near[dz + 1, 3, row:row + cy]
                    far_slope = slopes[dz + 1, row:row + cy]
                    square = sx * sx + sy * sy + sz * sz
                    inverse = lax.rsqrt(square)
                    distance = square * inverse
                    inside = 1.0 - square * (1.0 / RADIUS_SQ)
                    cut = inside * inside
                    cut_slope = inside * distance * (-4.0 / RADIUS_SQ)
                    growth = jnp.exp(2.0 - 2.0 * distance)
                    steep = 0.5 * growth * growth
                    coupling = (slope * far_weight + far_slope * weight) * (
                        growth * (cut_slope - 2.0 * cut)) + weight * far_weight * (
                        steep * (cut_slope - 4.0 * cut))
                    scale = coupling * inverse
                    force = [force[0] + scale * sx, force[1] + scale * sy, force[2] + scale * sz]
                    if last:
                        pair = pair + far_weight * (steep * cut)
            if last:
                for q in range(3):
                    force_ref[q, x] = force[q]
                energy_ref[x] = 0.5 * weight * pair - jnp.where(
                    weight > 0.0, slopes[3, start:start + cy], 0.0)
            else:
                for q in range(3):
                    mine[q][x] = here[q] + STEP * force[q]


def solution(mesh):
    counts = tuple(mesh.shape[axis] for axis in AXES)

    def body(displace, occupied, strength):
        sizes = occupied.shape
        cx, cy, cz = sizes
        pitch = cy + 4
        x_rows = up(3 * cx * cy + 2) + up(cx * cy)
        y_rows = up(6 * cx + 2) + up(2 * cx)
        rows = up(2 * (pitch + 1) + up((cx + 2) * pitch + cy + 3 - (pitch + 1)))
        f32 = jnp.float32
        vmem = pl.BlockSpec(memory_space=pltpu.VMEM)
        return pl.pallas_call(
            functools.partial(kernel, sizes, counts),
            out_shape=(pltpu.VMEM((3,) + sizes, f32), pltpu.VMEM(sizes, f32)),
            in_specs=[pl.BlockSpec(memory_space=pl.ANY)] * 3,
            out_specs=(vmem, vmem),
            scratch_shapes=[
                pltpu.VMEM((ITERS, x_rows, LANES), f32),
                pltpu.VMEM((ITERS, 2, y_rows, LANES), f32),
                pltpu.VMEM((ITERS, 2, 2, LANES), f32),
                pltpu.VMEM((ITERS, 2, x_rows, LANES), f32),
                pltpu.VMEM((ITERS, 3, 2, y_rows, LANES), f32),
                pltpu.VMEM((ITERS, 9, 2, 2, LANES), f32),
                pltpu.VMEM((LANES, LANES), f32),
                pltpu.VMEM((3, 4, rows, LANES), f32),
                pltpu.VMEM((9, 8, LANES), f32),
                pltpu.VMEM((4, rows, LANES), f32),
                pltpu.VMEM((3,) + sizes, f32),
                pltpu.VMEM(sizes, jnp.int32),
                pltpu.VMEM(sizes, f32),
                pltpu.SemaphoreType.DMA((len(NEAR),)),
                pltpu.SemaphoreType.DMA((2, len(NEAR))),
                pltpu.SemaphoreType.DMA((3,)),
            ],
            compiler_params=pltpu.CompilerParams(collective_id=0, has_side_effects=True),
        )(displace, occupied, strength)

    in_specs = (P(None, "gx", "gy", "gz"), P("gx", "gy", "gz"), P("gx", "gy", "gz"))
    out_specs = (P(None, "gx", "gy", "gz"), P("gx", "gy", "gz"))
    return jax.shard_map(body, mesh=mesh, in_specs=in_specs, out_specs=out_specs, check_vma=False)
```

```python
import functools

import jax
import jax.numpy as jnp
from jax import lax
from jax.experimental import pallas as pl
from jax.experimental.pallas import tpu as pltpu
from jax.sharding import PartitionSpec as P

ITERS = 3
RADIUS_SQ = 4.84
STEP = 0.02
AXES = ("gx", "gy", "gz")
MESH = pl.DeviceIdType.MESH
LANES = 128
PLANE = [(dx, dy) for dx in (-1, 0, 1) for dy in (-1, 0, 1)]
NEAR = sorted(
    ((dx, dy, dz) for dx, dy in PLANE for dz in (-1, 0, 1) if (dx, dy, dz) != (0, 0, 0)),
    key=lambda o: (-sum(abs(a) for a in o), o),
)


def minus(o):
    return tuple(-a for a in o)


def up(rows):
    return -(-rows // 8) * 8


def kernel(sizes, counts, disp_hbm, occ_hbm, str_hbm, force_ref, energy_ref,
           xs, ys, zs, xl, yl, zl, stage, near, cols, slopes, disp_ref, occ_ref, str_ref,
           zero, zero_row, sink_x, sink_y, sink_z, tally, send_sem, recv_sem, load_sem):
    cx, cy, cz = sizes
    pitch = cy + 4
    group = LANES // 4
    xu, yu = 3 * cx * cy, 3 * cx * 2
    xpanel, ypanel = xu, yu
    xw, yw = up(xu + 2), up(yu + 2)
    x_rows = (xs.shape[1], xw)
    y_rows = (ys.shape[2], yw)

    loads = [pltpu.make_async_copy(disp_hbm, disp_ref, load_sem.at[0]),
             pltpu.make_async_copy(occ_hbm, occ_ref, load_sem.at[1]),
             pltpu.make_async_copy(str_hbm, str_ref, load_sem.at[2])]
    for load in loads:
        load.start()

    me = [lax.axis_index(axis) for axis in AXES]
    there = [[None if s == 0 else (m + s >= 0) & (m + s < n) for s in (-1, 0, 1)]
             for m, n in zip(me, counts)]

    def exists(o):
        tests = [there[a][o[a] + 1] for a in range(3) if o[a] != 0]
        return functools.reduce(lambda p, q: p & q, tests)

    def target(o):
        return {AXES[a]: me[a] + o[a] for a in range(3)}

    barrier = pltpu.get_barrier_semaphore()
    for o in NEAR:
        @pl.when(exists(o))
        def _(o=o):
            pl.semaphore_signal(barrier, inc=1, device_id=target(o), device_id_type=MESH)
    spans = [1 + (m > 0).astype(jnp.int32) + (m < n - 1).astype(jnp.int32)
             for m, n in zip(me, counts)]

    def ends(t, o):
        back = minus(o)
        if o[2] != 0:
            side = 0 if o[2] == 1 else 1
            src = zs.at[t, side]
            dst = zl.at[t, PLANE.index(back[:2]), side]
        elif o[1] != 0:
            rows = y_rows[0] if t == 0 else y_rows[1]
            side = 0 if o[1] == 1 else 1
            src = ys.at[t, side, pl.ds(0, rows)]
            dst = yl.at[t, back[0] + 1, side, pl.ds(0, rows)]
        else:
            rows = x_rows[0] if t == 0 else x_rows[1]
            src = xs.at[t, pl.ds(0, rows)]
            dst = xl.at[t, 0 if o[0] == 1 else 1, pl.ds(0, rows)]
        return pltpu.make_async_remote_copy(
            src_ref=src, dst_ref=dst, send_sem=send_sem,
            recv_sem=recv_sem.at[t % 2], device_id=target(o), device_id_type=MESH)

    def fill(t, o):
        if o[2] != 0:
            j, side = PLANE.index(o[:2]), 0 if o[2] == -1 else 1
            src, spot, sink = zero_row, zl.at[t, j, side], sink_z.at[j, side]
        elif o[1] != 0:
            rows = pl.ds(0, y_rows[0] if t == 0 else y_rows[1])
            side = 0 if o[1] == -1 else 1
            src, spot = zero.at[rows], yl.at[t, o[0] + 1, side, rows]
            sink = sink_y.at[o[0] + 1, side, rows]
        else:
            rows = pl.ds(0, x_rows[0] if t == 0 else x_rows[1])
            side = 0 if o[0] == -1 else 1
            src, spot, sink = zero.at[rows], xl.at[t, side, rows], sink_x.at[side, rows]
        pltpu.make_async_copy(src, spot, recv_sem.at[t % 2]).start()
        pltpu.make_async_copy(src, sink, send_sem).start()

    zero[...] = jnp.zeros(zero.shape, jnp.float32)
    zero_row[...] = jnp.zeros(zero_row.shape, jnp.float32)
    stage[...] = jnp.zeros(stage.shape, jnp.float32)
    near[...] = jnp.zeros(near.shape, jnp.float32)
    cols[...] = jnp.zeros(cols.shape, jnp.float32)

    for load in loads:
        load.wait()
    mine = [[disp_ref[q, x] for x in range(cx)] for q in range(3)]
    mine.append([occ_ref[x].astype(jnp.float32) * str_ref[x] for x in range(cx)])

    lane = lax.broadcasted_iota(jnp.int32, (8, LANES), 1)
    sub = lax.broadcasted_iota(jnp.int32, (8, LANES), 0)
    in_group = lax.rem(lax.rem(lane, group), pitch)
    depth = (lax.rem(sub, 4) - 1).astype(jnp.float32)
    middle = lax.rem(sub, 4) == 1
    hollow = lax.rem(sub, 4) == 3

    def moved(value, amount, axis=1):
        amount %= value.shape[axis]
        return value if amount == 0 else pltpu.roll(value, amount, axis)

    for t in range(ITERS):
        last = t == ITERS - 1
        for q in range(4):
            for x in range(cx):
                if q < 3 or t == 0:
                    stage[q * group + x * pitch + 2:q * group + x * pitch + 2 + cy] = mine[q][x]
        flipped = jnp.transpose(stage[...])
        head, tail = flipped[0:2], flipped[cz - 2:cz]
        first, final = flipped[0:1], flipped[cz - 1:cz]
        zs[t, 0] = tail
        zs[t, 1] = head
        for side in range(2):
            for q in range(4):
                if q == 3 and t > 0:
                    continue
                for x in range(cx):
                    base = (q * cx + x) * 2 if q < 3 else yw + x * 2
                    piece = mine[q][x]
                    ys[t, side, base:base + 2] = piece[cy - 2:cy] if side == 0 else piece[0:2]
            ys[t, side, ypanel:ypanel + 1] = first
            ys[t, side, ypanel + 1:ypanel + 2] = final
        for q in range(4):
            if q == 3 and t > 0:
                continue
            for x in range(cx):
                base = (q * cx + x) * cy if q < 3 else xw + x * cy
                xs[t, base:base + cy] = mine[q][x]
        xs[t, xpanel:xpanel + 1] = first
        xs[t, xpanel + 1:xpanel + 2] = final

        if t == 0:
            pl.semaphore_wait(barrier, spans[0] * spans[1] * spans[2] - 1)
        for o in NEAR:
            @pl.when(exists(o))
            def _(o=o):
                ends(t, o).start()

            @pl.when(jnp.logical_not(exists(o)))
            def _(o=o):
                fill(t, o)
        pick = 0 if t == 0 else 1
        bytes_of = tally.at[pl.ds(0, (2 * x_rows[pick] + 6 * y_rows[pick] + 36) // 4)]
        pltpu.make_async_copy(bytes_of, bytes_of, recv_sem.at[t % 2]).wait()
        pltpu.make_async_copy(bytes_of, bytes_of, send_sem).wait()

        quantities = range(4) if t == 0 else range(3)
        for q in quantities:
            for dx in (-1, 0, 1):
                for x in range(cx):
                    row = (cx * (dx + 1) + x) * pitch
                    if dx == 0:
                        piece = mine[q][x]
                    else:
                        base = (q * cx + x) * cy if q < 3 else xw + x * cy
                        piece = xl[t, 0 if dx == -1 else 1, base:base + cy]
                    near[1, q, row + 2:row + 2 + cy] = piece
                    base = (q * cx + x) * 2 if q < 3 else yw + x * 2
                    near[1, q, row:row + 2] = yl[t, dx + 1, 0, base:base + 2]
                    near[1, q, row + 2 + cy:row + 4 + cy] = yl[t, dx + 1, 1, base:base + 2]
        for j, (dx, dy) in enumerate(PLANE):
            cols[j, 0:2] = zl[t, j, 0]
            cols[j, 5:7] = zl[t, j, 1]
            if dy != 0:
                a = yl[t, dx + 1, 0 if dy == -1 else 1, ypanel:ypanel + 1]
                b = yl[t, dx + 1, 0 if dy == -1 else 1, ypanel + 1:ypanel + 2]
            elif dx != 0:
                a = xl[t, 0 if dx == -1 else 1, xpanel:xpanel + 1]
                b = xl[t, 0 if dx == -1 else 1, xpanel + 1:xpanel + 2]
            else:
                a, b = first, final
            cols[j, 2:3] = a
            cols[j, 4:5] = b
        joined = []
        for dx in (-1, 0, 1):
            low, mid, high = (cols[PLANE.index((dx, dy))] for dy in (-1, 0, 1))
            joined.append(jnp.where(in_group < 2, moved(low, -cy),
                                    jnp.where(in_group < 2 + cy, mid, moved(high, cy))))
        wide = cx * pitch
        edge = []
        for q in range(4):
            value = jnp.zeros((8, LANES), jnp.float32)
            for i in (2, 1, 0):
                value = jnp.where(lane < wide * (i + 1),
                                  moved(joined[i], wide * i - group * q),
                                  value if i < 2 else 0.0)
            edge.append(value)

        turned = jnp.transpose(jnp.concatenate(edge, axis=0))
        rows = near.shape[2]
        wide_lane = lax.broadcasted_iota(jnp.int32, (rows, LANES), 1)
        for q in quantities:
            here = near[1, q]
            before = turned[0:rows, 8 * q + 1:8 * q + 2]
            after = turned[0:rows, 8 * q + 5:8 * q + 6]
            near[0, q] = jnp.where(wide_lane == 0, before, moved(here, 1))
            near[2, q] = jnp.where(wide_lane == cz - 1, after, moved(here, -1))

        center = [jnp.where(sub < 4, e[1:2], e[5:6]) for e in edge[:3]]
        total = jnp.zeros((8, LANES), jnp.float32)
        for dx, dy in PLANE:
            shift = -(dx * pitch + dy)
            far = [moved(e, shift) for e in edge]
            sx = far[0] - (center[0] - dx)
            sy = far[1] - (center[1] - dy)
            sz = far[2] - (center[2] - depth)
            square = sx * sx + sy * sy + sz * sz
            far_weight = far[3]
            if (dx, dy) == (0, 0):
                square = jnp.where(middle | hollow, 1.0, square)
                far_weight = jnp.where(middle | hollow, 0.0, far_weight)
            distance = square * lax.rsqrt(square)
            inside = 1.0 - square * (1.0 / RADIUS_SQ)
            total = total + far_weight * (jnp.exp(2.0 - 2.0 * distance) * (inside * inside))
        total = total + moved(total, 1, 0) + moved(total, -1, 0)
        edge_slope = jnp.where((edge[3] > 0.0) & middle, -0.5 * lax.rsqrt(1.0 + total), 0.0)
        turned_slope = jnp.transpose(edge_slope)

        begin = pitch + 1
        chunk = 16
        extent = up((cx + 2) * pitch + cy + 3 - begin)
        for start in range(begin, begin + extent, chunk):
            size = min(chunk, begin + extent - start)
            base = [[near[1, q, start:start + size] - s for s in (-1.0, 0.0, 1.0)] for q in range(3)]
            total = jnp.zeros((size, LANES), jnp.float32)
            for dx, dy in PLANE:
                row = start + dx * pitch + dy
                for dz in (-1, 0, 1):
                    if (dx, dy, dz) == (0, 0, 0):
                        continue
                    sx = near[dz + 1, 0, row:row + size] - base[0][dx + 1]
                    sy = near[dz + 1, 1, row:row + size] - base[1][dy + 1]
                    sz = near[dz + 1, 2, row:row + size] - base[2][dz + 1]
                    square = sx * sx + sy * sy + sz * sz
                    distance = square * lax.rsqrt(square)
                    inside = 1.0 - square * (1.0 / RADIUS_SQ)
                    total = total + near[dz + 1, 3, row:row + size] * (
                        jnp.exp(2.0 - 2.0 * distance) * (inside * inside))
            root = lax.rsqrt(1.0 + total)
            slope = jnp.where(near[1, 3, start:start + size] > 0.0, -0.5 * root, 0.0)
            slopes[1, start:start + size] = slope
            tall = lax.broadcasted_iota(jnp.int32, (size, LANES), 1)
            slopes[0, start:start + size] = jnp.where(
                tall == 0, turned_slope[start:start + size, 1:2], moved(slope, 1))
            slopes[2, start:start + size] = jnp.where(
                tall == cz - 1, turned_slope[start:start + size, 5:6], moved(slope, -1))
            if last:
                slopes[3, start:start + size] = (1.0 + total) * root

        for x in range(cx):
            start = (cx + x) * pitch + 2
            here = [mine[q][x] for q in range(3)]
            base = [[h - s for s in (-1.0, 0.0, 1.0)] for h in here]
            weight = mine[3][x]
            slope = slopes[1, start:start + cy]
            force = [jnp.zeros((cy, LANES), jnp.float32) for _ in range(3)]
            pair = jnp.zeros((cy, LANES), jnp.float32)
            for dx, dy in PLANE:
                row = start + dx * pitch + dy
                for dz in (-1, 0, 1):
                    if (dx, dy, dz) == (0, 0, 0):
                        continue
                    sx = near[dz + 1, 0, row:row + cy] - base[0][dx + 1]
                    sy = near[dz + 1, 1, row:row + cy] - base[1][dy + 1]
                    sz = near[dz + 1, 2, row:row + cy] - base[2][dz + 1]
                    far_weight = near[dz + 1, 3, row:row + cy]
                    far_slope = slopes[dz + 1, row:row + cy]
                    square = sx * sx + sy * sy + sz * sz
                    inverse = lax.rsqrt(square)
                    distance = square * inverse
                    inside = 1.0 - square * (1.0 / RADIUS_SQ)
                    cut = inside * inside
                    cut_slope = inside * distance * (-4.0 / RADIUS_SQ)
                    growth = jnp.exp(2.0 - 2.0 * distance)
                    steep = 0.5 * growth * growth
                    coupling = (slope * far_weight + far_slope * weight) * (
                        growth * (cut_slope - 2.0 * cut)) + weight * far_weight * (
                        steep * (cut_slope - 4.0 * cut))
                    scale = coupling * inverse
                    force = [force[0] + scale * sx, force[1] + scale * sy, force[2] + scale * sz]
                    if last:
                        pair = pair + far_weight * (steep * cut)
            if last:
                for q in range(3):
                    force_ref[q, x] = force[q]
                energy_ref[x] = 0.5 * weight * pair - jnp.where(
                    weight > 0.0, slopes[3, start:start + cy], 0.0)
            else:
                for q in range(3):
                    mine[q][x] = here[q] + STEP * force[q]


def solution(mesh):
    counts = tuple(mesh.shape[axis] for axis in AXES)

    def body(displace, occupied, strength):
        sizes = occupied.shape
        cx, cy, cz = sizes
        pitch = cy + 4
        x_rows = up(3 * cx * cy + 2) + up(cx * cy)
        y_rows = up(6 * cx + 2) + up(2 * cx)
        rows = up(2 * (pitch + 1) + up((cx + 2) * pitch + cy + 3 - (pitch + 1)))
        f32 = jnp.float32
        vmem = pl.BlockSpec(memory_space=pltpu.VMEM)
        return pl.pallas_call(
            functools.partial(kernel, sizes, counts),
            out_shape=(pltpu.VMEM((3,) + sizes, f32), pltpu.VMEM(sizes, f32)),
            in_specs=[pl.BlockSpec(memory_space=pl.ANY)] * 3,
            out_specs=(vmem, vmem),
            scratch_shapes=[
                pltpu.VMEM((ITERS, x_rows, LANES), f32),
                pltpu.VMEM((ITERS, 2, y_rows, LANES), f32),
                pltpu.VMEM((ITERS, 2, 2, LANES), f32),
                pltpu.VMEM((ITERS, 2, x_rows, LANES), f32),
                pltpu.VMEM((ITERS, 3, 2, y_rows, LANES), f32),
                pltpu.VMEM((ITERS, 9, 2, 2, LANES), f32),
                pltpu.VMEM((LANES, LANES), f32),
                pltpu.VMEM((3, 4, rows, LANES), f32),
                pltpu.VMEM((9, 8, LANES), f32),
                pltpu.VMEM((4, rows, LANES), f32),
                pltpu.VMEM((3,) + sizes, f32),
                pltpu.VMEM(sizes, jnp.int32),
                pltpu.VMEM(sizes, f32),
                pltpu.VMEM((x_rows, LANES), f32),
                pltpu.VMEM((2, LANES), f32),
                pltpu.VMEM((2, x_rows, LANES), f32),
                pltpu.VMEM((3, 2, y_rows, LANES), f32),
                pltpu.VMEM((9, 2, 2, LANES), f32),
                pltpu.VMEM(((2 * x_rows + 6 * y_rows + 36) // 4, 4, LANES), f32),
                pltpu.SemaphoreType.DMA,
                pltpu.SemaphoreType.DMA((2,)),
                pltpu.SemaphoreType.DMA((3,)),
            ],
            compiler_params=pltpu.CompilerParams(collective_id=0, has_side_effects=True),
        )(displace, occupied, strength)

    in_specs = (P(None, "gx", "gy", "gz"), P("gx", "gy", "gz"), P("gx", "gy", "gz"))
    out_specs = (P(None, "gx", "gy", "gz"), P("gx", "gy", "gz"))
    return jax.shard_map(body, mesh=mesh, in_specs=in_specs, out_specs=out_specs, check_vma=False)
```
